32 devices in a mesh: row: 8 (over y, x, core), col: 4 (over z).
Axes of the slice: x: 2, y: 2, z: 4, core: 2. Of those that a mesh axis runs over, the one named last changes fastest.
Arguments:
- entities: bfloat16 [2, 32768, 200], P(None, ('row', 'col')), may hold values from -2.390625 to 2.390625
- relations: bfloat16 [2, 1024, 200], replicated, may hold values from -6 to 6
- src_index: int32 [131072], P(('row', 'col')), may hold values from 0 to 4095
- dst_index: int32 [131072], P(('row', 'col')), may hold values from 0 to 8191
- rel_index: int32 [131072], P(('row', 'col')), may hold values from 0 to 1023
- neg_block: int32 [256], P(('row', 'col')), may hold values from 0 to 15
Outputs:
- edge_loss: float32 [131072], P(('row', 'col'))
- relation_grad: float32 [2, 1024, 200], P(None, ('row', 'col'))
The draws below stay inside these ranges and needn't reach their ends.
All inputs are finite; a program needn't handle non-finite values.
Results may differ from the reference program's by a relative error of at most 0.0018.
Values may be sent and summed in bfloat16 or wider, within the bound.
A program may use at most 128 MiB of HBM per device.

```python
import jax
import jax.numpy as jnp
from jax import lax

DIM = 200
NREL = 1024
ENT_DEV = 1024
EDGE_DEV = 4096
GROUP = 512
NEGB = 512
NENT = 32768
EDGES = 131072
N_ROW = 8
N_COL = 4


def place_ends(entries, rng, least, largest):
    longest = entries.shape.index(max(entries.shape))
    spots = []
    for shift in (0, 1):
        where = [jax.random.randint(jax.random.fold_in(rng, axis), (), 0, length) for axis, length in enumerate(entries.shape)]
        where[longest] = (where[longest] + shift) % entries.shape[longest]
        spots.append(tuple(where))
    return entries.at[spots[0]].set(least).at[spots[1]].set(largest)


def block_levels(rng, shape, cuts, low, high):
    loudness, own = 1.0, jax.random.fold_in(rng, 6)
    for dim, parts in cuts:
        steps = jnp.exp(jax.random.uniform(jax.random.fold_in(own, dim), (parts,), jnp.float32, low / len(cuts), high / len(cuts)))
        loudness = loudness * jnp.repeat(steps, shape[dim] // parts).reshape([-1 if axis == dim else 1 for axis in range(len(shape))])
    return loudness


def centred(stream_key, extent, width, bound, pieces=(), kind=jnp.bfloat16):
    level = block_levels(stream_key, extent, pieces, -0.22, 0.18) if pieces else 1.0
    array = jax.random.normal(stream_key, extent, jnp.float32) * width * level
    return jnp.minimum(jnp.maximum(array, -bound), bound).astype(kind)


def setup_inputs(seed: int = 0) -> dict:
    key_of = jax.random.split(jax.random.key(seed), 7)
    return {
        "entities": centred(key_of[0], (2, NENT, DIM), 0.4, 2.390625, ((1, 32),)),
        "relations": centred(key_of[1], (2, NREL, DIM), 1.0, 6.0),
        "src_index": place_ends(jax.random.randint(key_of[2], (EDGES,), 0, N_COL * ENT_DEV), jax.random.fold_in(key_of[2], 1), 0, (N_COL * ENT_DEV) - 1).astype(jnp.int32),
        "dst_index": place_ends(jax.random.randint(key_of[3], (EDGES,), 0, N_ROW * ENT_DEV), jax.random.fold_in(key_of[3], 1), 0, (N_ROW * ENT_DEV) - 1).astype(jnp.int32),
        "rel_index": place_ends(jax.random.randint(key_of[4], (EDGES,), 0, NREL), jax.random.fold_in(key_of[4], 1), 0, NREL - 1).astype(jnp.int32),
        "neg_block": place_ends(jax.random.randint(key_of[5], (EDGES // GROUP,), 0, N_ROW * ENT_DEV // NEGB), jax.random.fold_in(key_of[5], 1), 0, (N_ROW * ENT_DEV // NEGB) - 1).astype(jnp.int32),
    }


def bucket_terms(picked_src, picked_dst, negatives, relations, rel_ids):
    onehot = (rel_ids[:, None] == jnp.arange(relations.shape[1], dtype=jnp.int32)[None, :]).astype(jnp.bfloat16)
    rel_re = jnp.dot(onehot, relations[0], preferred_element_type=jnp.float32)
    rel_im = jnp.dot(onehot, relations[1], preferred_element_type=jnp.float32)
    src_re = picked_src[0].astype(jnp.float32)
    src_im = picked_src[1].astype(jnp.float32)
    dst_re = picked_dst[0].astype(jnp.float32)
    dst_im = picked_dst[1].astype(jnp.float32)
    query_re = src_re * rel_re - src_im * rel_im
    query_im = src_re * rel_im + src_im * rel_re
    pos_score = jnp.sum(query_re * dst_re, 1) + jnp.sum(query_im * dst_im, 1)
    groups = negatives.shape[1]
    dim = query_re.shape[1]
    qre_f = query_re.astype(jnp.bfloat16).astype(jnp.float32).reshape(groups, -1, dim)
    qim_f = query_im.astype(jnp.bfloat16).astype(jnp.float32).reshape(groups, -1, dim)
    neg_re = negatives[0].astype(jnp.float32)
    neg_im = negatives[1].astype(jnp.float32)
    neg_score = jnp.einsum("kcd,knd->kcn", qre_f, neg_re, precision=lax.Precision.HIGHEST) + jnp.einsum("kcd,knd->kcn", qim_f, neg_im, precision=lax.Precision.HIGHEST)
    edge_loss = jax.nn.softplus(-pos_score) + jnp.mean(jax.nn.softplus(neg_score), -1).reshape(-1)
    weights = (jax.nn.sigmoid(neg_score) / NEGB).astype(jnp.bfloat16).astype(jnp.float32)
    gneg_re = jnp.einsum("kcn,knd->kcd", weights, neg_re, precision=lax.Precision.HIGHEST).reshape(-1, dim)
    gneg_im = jnp.einsum("kcn,knd->kcd", weights, neg_im, precision=lax.Precision.HIGHEST).reshape(-1, dim)
    pull = jax.nn.sigmoid(-pos_score)[:, None]
    grad_re = gneg_re - pull * dst_re
    grad_im = gneg_im - pull * dst_im
    term_re = (grad_re * src_re + grad_im * src_im).astype(jnp.bfloat16)
    term_im = (grad_im * src_re - grad_re * src_im).astype(jnp.bfloat16)
    dims = (((0,), (0,)), ((), ()))
    rel_grad = jnp.stack([lax.dot_general(onehot, term_re, dims, preferred_element_type=jnp.float32), lax.dot_general(onehot, term_im, dims, preferred_element_type=jnp.float32)], 0)
    return edge_loss, rel_grad


def reference(entities, relations, src_index, dst_index, rel_index, neg_block):
    dim = entities.shape[2]
    grid_rows = entities.reshape(2, N_ROW, N_COL, ENT_DEV, dim)
    groups = EDGE_DEV // GROUP

    def visit(accum, device):
        row_pos = device // N_COL
        col_pos = device % N_COL
        source_rows = lax.dynamic_index_in_dim(grid_rows, row_pos, 1, keepdims=False).reshape(2, N_COL * ENT_DEV, dim)
        target_rows = lax.dynamic_index_in_dim(grid_rows, col_pos, 2, keepdims=False).reshape(2, N_ROW * ENT_DEV, dim)
        sources = lax.dynamic_slice_in_dim(src_index, (device * EDGE_DEV).astype(jnp.int32), EDGE_DEV)
        targets = lax.dynamic_slice_in_dim(dst_index, (device * EDGE_DEV).astype(jnp.int32), EDGE_DEV)
        rel_ids = lax.dynamic_slice_in_dim(rel_index, (device * EDGE_DEV).astype(jnp.int32), EDGE_DEV)
        block_ids = lax.dynamic_slice_in_dim(neg_block, (device * groups).astype(jnp.int32), groups)
        picked_src = jnp.take(source_rows, sources, axis=1)
        picked_dst = jnp.take(target_rows, targets, axis=1)
        negatives = jnp.take(target_rows.reshape(2, -1, NEGB, dim), block_ids, axis=1)
        edge_loss, rel_grad = bucket_terms(picked_src, picked_dst, negatives, relations, rel_ids)
        return accum + rel_grad, edge_loss

    rel_total, losses = lax.scan(visit, jnp.zeros((2, NREL, dim), jnp.float32), jnp.arange(N_ROW * N_COL, dtype=jnp.int32))
    return losses.reshape(-1), rel_total
```

```python
import functools

import jax
import jax.numpy as jnp
from jax import lax
from jax.experimental import pallas as pl
from jax.experimental.pallas import tpu as pltpu
from jax.sharding import PartitionSpec as P

NEGB = 512
LANE = 128
WIDE = 256
VMEM_CAP = 67_043_328
MESH = pl.DeviceIdType.MESH
F32 = jnp.float32
BF16 = jnp.bfloat16


def spread_kernel(n_row, n_col, ent, src_out, dst_out, loc_sem, col_s, col_r, row_s, row_r, pair_s, pair_r):
    r, c = lax.axis_index("row"), lax.axis_index("col")
    chips = n_row // 2
    chip, core = r // 2, r % 2
    mate = chip * 2 + (1 - core)

    barrier = pltpu.get_barrier_semaphore()
    peers = [(r, (c + k) % n_col) for k in range(1, n_col)]
    peers += [(((chip + k) % chips) * 2 + core, c) for k in range(1, chips)]
    peers += [(mate, c)]
    for peer in peers:
        pl.semaphore_signal(barrier, inc=1, device_id=peer, device_id_type=MESH)
    pl.semaphore_wait(barrier, len(peers))

    sends = []
    for k in range(1, max(n_col, chips)):
        if k < n_col:
            sends.append(
                pltpu.make_async_remote_copy(
                    src_ref=ent, dst_ref=src_out.at[c], send_sem=col_s.at[k], recv_sem=col_r.at[k],
                    device_id=(r, (c + k) % n_col), device_id_type=MESH,
                )
            )
        if k < chips:
            sends.append(
                pltpu.make_async_remote_copy(
                    src_ref=ent, dst_ref=dst_out.at[r], send_sem=row_s.at[k], recv_sem=row_r.at[k],
                    device_id=(((chip + k) % chips) * 2 + core, c), device_id_type=MESH,
                )
            )
    sends.append(
        pltpu.make_async_remote_copy(
            src_ref=ent, dst_ref=dst_out.at[r], send_sem=pair_s.at[0], recv_sem=pair_r.at[0],
            device_id=(mate, c), device_id_type=MESH,
        )
    )
    for send in sends:
        send.start()
    local = [
        pltpu.make_async_copy(ent, src_out.at[c], loc_sem.at[0]),
        pltpu.make_async_copy(ent, dst_out.at[r], loc_sem.at[1]),
    ]
    for copy in local:
        copy.start()
    relays = []
    for k in range(1, chips):
        origin = ((chip + chips - k) % chips) * 2 + core
        pltpu.make_async_remote_copy(
            src_ref=ent, dst_ref=dst_out.at[origin], send_sem=row_s.at[k], recv_sem=row_r.at[k],
            device_id=(mate, c), device_id_type=MESH,
        ).wait_recv()
        relay = pltpu.make_async_remote_copy(
            src_ref=dst_out.at[origin], dst_ref=dst_out.at[origin], send_sem=pair_s.at[k], recv_sem=pair_r.at[k],
            device_id=(mate, c), device_id_type=MESH,
        )
        relay.start()
        relays.append(relay)
    for k in range(1, n_col):
        pltpu.make_async_remote_copy(
            src_ref=ent, dst_ref=src_out.at[(c + n_col - k) % n_col], send_sem=col_s.at[k], recv_sem=col_r.at[k],
            device_id=(mate, c), device_id_type=MESH,
        ).wait_recv()
    for send in sends:
        send.wait_send()
    sends[-1].wait_recv()
    for relay in relays:
        relay.wait()
    for copy in local:
        copy.wait()


def spread(n_row, n_col, ent):
    chips = n_row // 2
    dma = pltpu.SemaphoreType.DMA
    return pl.pallas_call(
        functools.partial(spread_kernel, n_row, n_col),
        name="spread",
        out_shape=(
            jax.ShapeDtypeStruct((n_col,) + ent.shape, ent.dtype),
            jax.ShapeDtypeStruct((n_row,) + ent.shape, ent.dtype),
        ),
        in_specs=[pl.BlockSpec(memory_space=pltpu.VMEM)],
        out_specs=(pl.BlockSpec(memory_space=pltpu.HBM), pl.BlockSpec(memory_space=pltpu.HBM)),
        scratch_shapes=[
            dma((2,)), dma((n_col,)), dma((n_col,)), dma((chips,)), dma((chips,)), dma((chips,)), dma((chips,)),
        ],
        compiler_params=pltpu.CompilerParams(collective_id=0, has_side_effects=True),
    )(ent)


def gather_sum_kernel(n_row, n_col, acc, out, pair_buf, sums, got, pair_s, pair_r, far_s, far_r):
    r, c = lax.axis_index("row"), lax.axis_index("col")
    chips = n_row // 2
    chip, core = r // 2, r % 2
    mate = chip * 2 + (1 - core)
    steps = [(a, b) for a in range(chips) for b in range(n_col) if a or b]
    goal = lambda a, b: (((chip + a) % chips) * 2 + core, (c + b) % n_col)

    barrier = pltpu.get_barrier_semaphore()
    for a, b in steps:
        pl.semaphore_signal(barrier, inc=1, device_id=goal(a, b), device_id_type=MESH)
    pl.semaphore_signal(barrier, inc=1, device_id=(mate, c), device_id_type=MESH)
    pl.semaphore_wait(barrier, len(steps) + 1)

    pairs = []
    for j in range(chips):
        copy = pltpu.make_async_remote_copy(
            src_ref=acc.at[j, 1 - core], dst_ref=pair_buf.at[j], send_sem=pair_s.at[j], recv_sem=pair_r.at[j],
            device_id=(mate, c), device_id_type=MESH,
        )
        copy.start()
        pairs.append(copy)
    for j in range(chips):
        pairs[j].wait_recv()
        sums[j] = acc[j, core] + pair_buf[j]
    sends = []
    for a, b in steps:
        send = pltpu.make_async_remote_copy(
            src_ref=sums.at[(chip + a) % chips, (c + b) % n_col], dst_ref=got.at[a, b],
            send_sem=far_s.at[a, b], recv_sem=far_r.at[a, b],
            device_id=goal(a, b), device_id_type=MESH,
        )
        send.start()
        sends.append(send)
    total = sums[chip, c]
    for send, (a, b) in zip(sends, steps):
        send.wait_recv()
        total = total + got[a, b]
    width = out.shape[2]
    out[0] = total[:, :width]
    out[1] = total[:, WIDE : WIDE + width]
    for send in sends:
        send.wait_send()
    for copy in pairs:
        copy.wait_send()


def gather_sum(n_row, n_col, acc, dim):
    chips = n_row // 2
    rows = acc.shape[0] // (n_row * n_col)
    wide = acc.shape[1]
    dma = pltpu.SemaphoreType.DMA
    return pl.pallas_call(
        functools.partial(gather_sum_kernel, n_row, n_col),
        name="gather_sum",
        out_shape=jax.ShapeDtypeStruct((2, rows, dim), F32),
        in_specs=[pl.BlockSpec(memory_space=pltpu.VMEM)],
        out_specs=pl.BlockSpec(memory_space=pltpu.VMEM),
        scratch_shapes=[
            pltpu.VMEM((chips, n_col, rows, wide), F32),
            pltpu.VMEM((chips, n_col, rows, wide), F32),
            pltpu.VMEM((chips, n_col, rows, wide), F32),
            dma((chips,)), dma((chips,)), dma((chips, n_col)), dma((chips, n_col)),
        ],
        compiler_params=pltpu.CompilerParams(collective_id=1, has_side_effects=True),
    )(acc.reshape(chips, 2, n_col, rows, wide))


def edge_kernel(
    group, src_i, dst_i, rel_i, neg_i, rel_row, rel_tab, src_all, dst_all,
    loss, acc, stage, s_tab, o_tab, w_tab, gs, go, gw, neg, qb, pos, term, stage_sem, neg_sem,
):
    n_src, n_dst = src_all.shape[0], dst_all.shape[0]
    ent = src_all.shape[2]
    n_rel = rel_tab.shape[1]
    groups = neg_i.shape[0]
    per = ent // NEGB
    sub = 128

    def neg_copy(g):
        b = neg_i[g]
        return pltpu.make_async_copy(
            dst_all.at[b // per, :, pl.ds(pl.multiple_of((b % per) * NEGB, NEGB), NEGB), :],
            neg.at[g % 2], neg_sem.at[g % 2],
        )

    def fill(table, base, read, rows):
        def step(i, carry):
            row = pl.multiple_of(i * sub, sub)
            for part in range(2):
                for half in range(2):
                    piece = read(part, row, half).astype(F32)
                    table[pl.ds(base + row * 4 + part * 2 + half, sub, stride=4), :] = piece
            return carry

        lax.fori_loop(0, rows // sub, step, 0)

    def load(all_ref, table, count):
        def copy(i):
            return pltpu.make_async_copy(all_ref.at[i], stage.at[i % 2], stage_sem.at[i % 2])

        copy(0).start()

        def step(i, carry):
            @pl.when(i + 1 < count)
            def _():
                copy(i + 1).start()

            copy(i).wait()
            slot = i % 2
            fill(
                table, i * (ent * 4),
                lambda part, row, half: stage[slot, part, pl.ds(row, sub), half * LANE : (half + 1) * LANE], ent,
            )
            return carry

        lax.fori_loop(0, count, step, 0)

    neg_copy(0).start()
    fill(w_tab, 0, lambda part, row, half: rel_tab[part, pl.ds(row, sub), half * LANE : (half + 1) * LANE], n_rel)
    load(src_all, s_tab, n_src)
    load(dst_all, o_tab, n_dst)

    eye = lax.broadcasted_iota(jnp.int32, (sub, LANE), 0) == lax.broadcasted_iota(jnp.int32, (sub, LANE), 1)
    nt = (((1,), (1,)), ((), ()))

    def one_group(g, carry):
        @pl.when(g + 1 < groups)
        def _():
            neg_copy(g + 1).start()

        def pick(i, inner):
            got = []
            for u in range(8):
                e = i * 8 + u
                a = pl.multiple_of(src_i[g * group + e] * 4, 4)
                b = pl.multiple_of(dst_i[g * group + e] * 4, 4)
                k = pl.multiple_of(rel_i[g * group + e] * 4, 4)
                got.append((s_tab[pl.ds(a, 4), :], o_tab[pl.ds(b, 4), :], w_tab[pl.ds(k, 4), :]))
            for u in range(8):
                at = pl.ds(pl.multiple_of((i * 8 + u) * 4, 4), 4)
                gs[at, :], go[at, :], gw[at, :] = got[u]
            return inner

        lax.fori_loop(0, group // 8, pick, 0)

        qrows = 32

        def query(i, inner):
            row = pl.multiple_of(i * qrows, qrows)
            score = None
            for half in range(2):
                part = lambda ref, p: ref[pl.ds(row * 4 + p * 2 + half, qrows, stride=4), :]
                sr, si, wr, wi = part(gs, 0), part(gs, 1), part(gw, 0), part(gw, 1)
                qr = sr * wr - si * wi
                qi = sr * wi + si * wr
                add = qr * part(go, 0) + qi * part(go, 1)
                score = add if score is None else score + add
                qb[pl.ds(row, qrows), half * LANE : (half + 1) * LANE] = qr.astype(BF16)
                qb[pl.ds(row, qrows), WIDE + half * LANE : WIDE + (half + 1) * LANE] = qi.astype(BF16)
            pos[pl.ds(row, qrows), :] = jnp.sum(score, 1, keepdims=True)
            return inner

        lax.fori_loop(0, group // qrows, query, 0)
        neg_copy(g).wait()
        slot = g % 2

        def block(i, inner):
            row = pl.multiple_of(i * sub, sub)
            rows = pl.ds(row, sub)
            n_re, n_im = neg[slot, 0], neg[slot, 1]
            score = lax.dot_general(qb[rows, :WIDE], n_re, nt, preferred_element_type=F32)
            score = score + lax.dot_general(qb[rows, WIDE:], n_im, nt, preferred_element_type=F32)
            small = jnp.exp(-jnp.abs(score))
            soft = jnp.maximum(score, 0.0) + jnp.log1p(small)
            weight = (jnp.where(score >= 0.0, 1.0, small) / (1.0 + small) * (1.0 / NEGB)).astype(BF16)
            p = pos[rows, :]
            p_small = jnp.exp(-jnp.abs(p))
            value = jnp.maximum(-p, 0.0) + jnp.log1p(p_small) + jnp.sum(soft, 1, keepdims=True) * (1.0 / NEGB)
            pull = jnp.where(p >= 0.0, p_small, 1.0) / (1.0 + p_small)
            loss[pl.ds(g * (group // sub) + i, 1), :] = jnp.sum(jnp.where(eye, value, 0.0), 0, keepdims=True)
            g_re = jnp.dot(weight, n_re, preferred_element_type=F32)
            g_im = jnp.dot(weight, n_im, preferred_element_type=F32)
            for half in range(2):
                part = lambda ref, q: ref[pl.ds(row * 4 + q * 2 + half, sub, stride=4), :]
                cols = slice(half * LANE, (half + 1) * LANE)
                d_re = g_re[:, cols] - pull * part(go, 0)
                d_im = g_im[:, cols] - pull * part(go, 1)
                s_re, s_im = part(gs, 0), part(gs, 1)
                at = pl.ds(pl.multiple_of(g * group + row, sub), sub)
                term[at, half * LANE : (half + 1) * LANE] = (d_re * s_re + d_im * s_im).astype(BF16)
                term[at, WIDE + half * LANE : WIDE + (half + 1) * LANE] = (d_im * s_re - d_re * s_im).astype(BF16)
            return inner

        lax.fori_loop(0, group // sub, block, 0)
        return carry

    lax.fori_loop(0, groups, one_group, 0)

    tile = 256
    edges = term.shape[0]

    def reduce(i, carry):
        row = pl.multiple_of(i * tile, tile)
        ids = lax.broadcasted_iota(jnp.int32, (tile, edges), 0) + row
        hot = jnp.where(ids == rel_row[...], 1.0, 0.0).astype(BF16)
        acc[pl.ds(row, tile), :] = jnp.dot(hot, term[...], preferred_element_type=F32)
        return carry

    lax.fori_loop(0, n_rel // tile, reduce, 0)


def edge_terms(src_all, dst_all, relations, src_index, dst_index, rel_index, neg_block):
    edges, groups = src_index.shape[0], neg_block.shape[0]
    group = edges // groups
    n_rel = relations.shape[1]
    ent = src_all.shape[2]
    smem = pl.BlockSpec(memory_space=pltpu.SMEM)
    vmem = pl.BlockSpec(memory_space=pltpu.VMEM)
    hbm = pl.BlockSpec(memory_space=pltpu.HBM)
    quad = 4
    return pl.pallas_call(
        functools.partial(edge_kernel, group),
        name="edge_terms",
        out_shape=(
            jax.ShapeDtypeStruct((edges // LANE, LANE), F32),
            jax.ShapeDtypeStruct((n_rel, 2 * WIDE), F32),
        ),
        in_specs=[smem, smem, smem, smem, vmem, vmem, hbm, hbm],
        out_specs=(vmem, vmem),
        scratch_shapes=[
            pltpu.VMEM((2, 2, ent, WIDE), BF16),
            pltpu.VMEM((src_all.shape[0] * ent * quad, LANE), F32),
            pltpu.VMEM((dst_all.shape[0] * ent * quad, LANE), F32),
            pltpu.VMEM((n_rel * quad, LANE), F32),
            pltpu.VMEM((group * quad, LANE), F32),
            pltpu.VMEM((group * quad, LANE), F32),
            pltpu.VMEM((group * quad, LANE), F32),
            pltpu.VMEM((2, 2, NEGB, WIDE), BF16),
            pltpu.VMEM((group, 2 * WIDE), BF16),
            pltpu.VMEM((group, 1), F32),
            pltpu.VMEM((edges, 2 * WIDE), BF16),
            pltpu.SemaphoreType.DMA((2,)),
            pltpu.SemaphoreType.DMA((2,)),
        ],
        compiler_params=pltpu.CompilerParams(vmem_limit_bytes=62 * 2**20),
    )(
        src_index, dst_index, rel_index, neg_block, rel_index.reshape(1, edges), relations, src_all, dst_all,
    )


def body(n_row, n_col, entities, relations, src_index, dst_index, rel_index, neg_block):
    dim = entities.shape[2]
    ent = entities.shape[1]
    pad = ((0, 0), (0, 0), (0, WIDE - dim))
    if (n_row + n_col) * ent * 4 * LANE * 4 > 36 * 2**20:
        return wide_body(entities, relations, src_index, dst_index, rel_index, neg_block)
    src_all, dst_all = spread(n_row, n_col, jnp.pad(entities, pad))
    edge_loss, acc = edge_terms(
        src_all, dst_all, jnp.pad(relations, pad), src_index, dst_index, rel_index, neg_block
    )
    grad = gather_sum(n_row, n_col, acc, dim)
    return edge_loss.reshape(-1), grad


def bucket_terms(picked_src, picked_dst, negatives, relations, rel_ids):
    onehot = (rel_ids[:, None] == jnp.arange(relations.shape[1], dtype=jnp.int32)[None, :]).astype(
        jnp.bfloat16
    )
    rel_re = jnp.dot(onehot, relations[0], preferred_element_type=jnp.float32)
    rel_im = jnp.dot(onehot, relations[1], preferred_element_type=jnp.float32)
    src_re = picked_src[0].astype(jnp.float32)
    src_im = picked_src[1].astype(jnp.float32)
    dst_re = picked_dst[0].astype(jnp.float32)
    dst_im = picked_dst[1].astype(jnp.float32)
    query_re = src_re * rel_re - src_im * rel_im
    query_im = src_re * rel_im + src_im * rel_re
    pos_score = jnp.sum(query_re * dst_re, 1) + jnp.sum(query_im * dst_im, 1)
    groups = negatives.shape[1]
    dim = query_re.shape[1]
    qre_b = query_re.astype(jnp.bfloat16).reshape(groups, -1, dim)
    qim_b = query_im.astype(jnp.bfloat16).reshape(groups, -1, dim)
    neg_score = jnp.einsum(
        "kcd,knd->kcn", qre_b, negatives[0], preferred_element_type=jnp.float32
    ) + jnp.einsum("kcd,knd->kcn", qim_b, negatives[1], preferred_element_type=jnp.float32)
    edge_loss = jax.nn.softplus(-pos_score) + jnp.mean(jax.nn.softplus(neg_score), -1).reshape(-1)
    weights = (jax.nn.sigmoid(neg_score) / NEGB).astype(jnp.bfloat16)
    gneg_re = jnp.einsum(
        "kcn,knd->kcd", weights, negatives[0], preferred_element_type=jnp.float32
    ).reshape(-1, dim)
    gneg_im = jnp.einsum(
        "kcn,knd->kcd", weights, negatives[1], preferred_element_type=jnp.float32
    ).reshape(-1, dim)
    pull = jax.nn.sigmoid(-pos_score)[:, None]
    grad_re = gneg_re - pull * dst_re
    grad_im = gneg_im - pull * dst_im
    term_re = (grad_re * src_re + grad_im * src_im).astype(jnp.bfloat16)
    term_im = (grad_im * src_re - grad_re * src_im).astype(jnp.bfloat16)
    dims = (((0,), (0,)), ((), ()))
    rel_grad = jnp.stack(
        [
            lax.dot_general(onehot, term_re, dims, preferred_element_type=jnp.float32),
            lax.dot_general(onehot, term_im, dims, preferred_element_type=jnp.float32),
        ],
        0,
    )
    return (edge_loss, rel_grad)


def wide_body(entities, relations, src_index, dst_index, rel_index, neg_block):
    dim = entities.shape[2]
    source_rows = lax.all_gather(entities, "col", axis=1, tiled=True)
    picked_src = jnp.take(source_rows, src_index, axis=1)
    target_rows = lax.all_gather(entities, "row", axis=1, tiled=True)
    picked_dst = jnp.take(target_rows, dst_index, axis=1)
    negatives = jnp.take(target_rows.reshape(2, -1, NEGB, dim), neg_block, axis=1)
    edge_loss, rel_grad = bucket_terms(picked_src, picked_dst, negatives, relations, rel_index)
    row_share = lax.psum_scatter(rel_grad, "row", scatter_dimension=1, tiled=True)
    grad_share = lax.psum_scatter(row_share, "col", scatter_dimension=1, tiled=True)
    return (edge_loss, grad_share)


def solution(mesh):
    placed = (
        P(None, ("row", "col"), None),
        P(),
        P(("row", "col")),
        P(("row", "col")),
        P(("row", "col")),
        P(("row", "col")),
    )
    return jax.shard_map(
        functools.partial(body, mesh.shape["row"], mesh.shape["col"]),
        mesh=mesh,
        in_specs=placed,
        out_specs=(P(("row", "col")), P(None, ("row", "col"), None)),
        check_vma=False,
    )
```

```python
import functools

import jax
import jax.numpy as jnp
from jax import lax
from jax.experimental import pallas as pl
from jax.experimental.pallas import tpu as pltpu
from jax.sharding import PartitionSpec as P

NEGB = 512
LANE = 128
WIDE = 256
MESH = pl.DeviceIdType.MESH
F32 = jnp.float32
BF16 = jnp.bfloat16


def spread_kernel(n_col, ent, src_out, dst_out, loc_sem, send_sem, recv_sem):
    r, c = lax.axis_index("row"), lax.axis_index("col")
    chip, core = r // 2, r % 2
    y, x = chip // 2, chip % 2
    row_of = lambda yy, xx: (yy * 2 + xx) * 2 + core
    xr, yr, dr = row_of(y, 1 - x), row_of(1 - y, x), row_of(1 - y, 1 - x)
    up, down, across = (c + 1) % n_col, (c + n_col - 1) % n_col, (c + 2) % n_col
    mate = (chip * 2 + (1 - core), c)
    above, below, xp, yp = (r, up), (r, down), (xr, c), (yr, c)

    barrier = pltpu.get_barrier_semaphore()
    peers = [mate, above, below, xp, yp]
    for peer in peers:
        pl.semaphore_signal(barrier, inc=1, device_id=peer, device_id_type=MESH)
    pl.semaphore_wait(barrier, len(peers))

    def copy(k, src, dst, peer):
        return pltpu.make_async_remote_copy(
            src_ref=src, dst_ref=dst, send_sem=send_sem.at[k], recv_sem=recv_sem.at[k],
            device_id=peer, device_id_type=MESH,
        )

    own = lambda p: ent.at[p]
    col = lambda i, p: src_out.at[i, p]
    row = lambda i, p: dst_out.at[i, p]
    started = []

    def start(k, src, dst, peer):
        move = copy(k, src, dst, peer)
        move.start()
        started.append(move)

    def arrive(k, dst):
        copy(k, own(0), dst, mate).wait_recv()

    start(0, own(0), col(c, 0), above)
    start(3, own(1), col(c, 1), below)
    start(6, own(0), row(r, 0), xp)
    start(9, own(1), row(r, 1), yp)
    start(1, own(1), col(c, 1), above)
    start(2, own(0), col(c, 0), below)
    start(7, own(1), row(r, 1), xp)
    start(8, own(0), row(r, 0), yp)
    start(12, own(0), row(r, 0), mate)
    start(19, own(1), row(r, 1), mate)
    local = [
        pltpu.make_async_copy(ent, src_out.at[c], loc_sem.at[0]),
        pltpu.make_async_copy(ent, dst_out.at[r], loc_sem.at[1]),
    ]
    for move in local:
        move.start()
    arrive(0, col(down, 0))
    start(4, col(down, 0), col(down, 0), above)
    arrive(3, col(up, 1))
    start(5, col(up, 1), col(up, 1), below)
    arrive(6, row(xr, 0))
    start(10, row(xr, 0), row(xr, 0), yp)
    arrive(9, row(yr, 1))
    start(11, row(yr, 1), row(yr, 1), xp)
    start(13, row(xr, 0), row(xr, 0), mate)
    start(16, row(yr, 1), row(yr, 1), mate)
    arrive(7, row(xr, 1))
    start(14, row(xr, 1), row(xr, 1), mate)
    arrive(8, row(yr, 0))
    start(15, row(yr, 0), row(yr, 0), mate)
    arrive(10, row(dr, 0))
    start(17, row(dr, 0), row(dr, 0), mate)
    arrive(11, row(dr, 1))
    start(18, row(dr, 1), row(dr, 1), mate)
    arrive(1, col(down, 1))
    arrive(2, col(up, 0))
    arrive(4, col(across, 0))
    arrive(5, col(across, 1))
    twin = lambda yy, xx: (yy * 2 + xx) * 2 + (1 - core)
    mx, my, md = twin(y, 1 - x), twin(1 - y, x), twin(1 - y, 1 - x)
    arrive(12, row(mate[0], 0))
    arrive(19, row(mate[0], 1))
    arrive(13, row(mx, 0))
    arrive(14, row(mx, 1))
    arrive(15, row(my, 0))
    arrive(16, row(my, 1))
    arrive(17, row(md, 0))
    arrive(18, row(md, 1))
    for move in started:
        move.wait_send()
    for move in local:
        move.wait()


def spread(n_row, n_col, ent):
    dma = pltpu.SemaphoreType.DMA
    return pl.pallas_call(
        functools.partial(spread_kernel, n_col),
        name="spread",
        out_shape=(
            jax.ShapeDtypeStruct((n_col,) + ent.shape, ent.dtype),
            jax.ShapeDtypeStruct((n_row,) + ent.shape, ent.dtype),
        ),
        in_specs=[pl.BlockSpec(memory_space=pltpu.VMEM)],
        out_specs=(pl.BlockSpec(memory_space=pltpu.HBM), pl.BlockSpec(memory_space=pltpu.HBM)),
        scratch_shapes=[dma((2,)), dma((20,)), dma((20,))],
        compiler_params=pltpu.CompilerParams(collective_id=0, has_side_effects=True),
    )(ent)


def gather_sum_kernel(n_col, acc, out, pair_buf, sa, sb, a1, b1, ta, tb, a2, b2, tot, got, send_sem, recv_sem):
    r, c = lax.axis_index("row"), lax.axis_index("col")
    chip, core = r // 2, r % 2
    y, x = chip // 2, chip % 2
    row_of = lambda yy, xx: (yy * 2 + xx) * 2 + core
    mate = (chip * 2 + (1 - core), c)
    xp, yp = (row_of(y, 1 - x), c), (row_of(1 - y, x), c)
    ring = [(r, (c + b) % n_col) for b in range(1, n_col)]

    barrier = pltpu.get_barrier_semaphore()
    peers = [mate, xp, yp] + ring
    for peer in peers:
        pl.semaphore_signal(barrier, inc=1, device_id=peer, device_id_type=MESH)
    pl.semaphore_wait(barrier, len(peers))

    started = []

    def start(k, src, dst, peer):
        move = pltpu.make_async_remote_copy(
            src_ref=src, dst_ref=dst, send_sem=send_sem.at[k], recv_sem=recv_sem.at[k],
            device_id=peer, device_id_type=MESH,
        )
        move.start()
        started.append(move)
        return move

    spots = [(yy, xx) for yy in range(2) for xx in range(2)]
    pairs = [start(k, acc.at[yy, xx, 1 - core], pair_buf.at[yy, xx], mate) for k, (yy, xx) in enumerate(spots)]
    for move, (yy, xx) in zip(pairs, spots):
        move.wait_recv()
        whole = acc[yy, xx, core] + pair_buf[yy, xx]
        sa[yy, xx] = whole[:, :, :WIDE]
        sb[yy, xx] = whole[:, :, WIDE:]
    move_a = start(4, sa.at[:, 1 - x], a1, xp)
    move_b = start(5, sb.at[1 - y], b1, yp)
    move_a.wait_recv()
    ta[0] = sa[1 - y, x] + a1[1 - y]
    next_a = start(6, ta.at[0], a2, yp)
    ta[1] = sa[y, x] + a1[y]
    move_b.wait_recv()
    tb[0] = sb[y, 1 - x] + b1[1 - x]
    next_b = start(7, tb.at[0], b2, xp)
    tb[1] = sb[y, x] + b1[x]
    next_a.wait_recv()
    tot[:, :, :WIDE] = ta[1] + a2[...]
    next_b.wait_recv()
    tot[:, :, WIDE:] = tb[1] + b2[...]
    hops = [start(8 + b, tot.at[peer[1]], got.at[b], peer) for b, peer in enumerate(ring)]
    total = tot[c]
    for b, move in enumerate(hops):
        move.wait_recv()
        total = total + got[b]
    width = out.shape[2]
    out[0] = total[:, :width]
    out[1] = total[:, WIDE : WIDE + width]
    for move in started:
        move.wait_send()


def gather_sum(n_row, n_col, acc, dim):
    rows = acc.shape[0] // (n_row * n_col)
    wide = acc.shape[1]
    dma = pltpu.SemaphoreType.DMA
    block = lambda *lead: pltpu.VMEM(lead + (n_col, rows, WIDE), F32)
    return pl.pallas_call(
        functools.partial(gather_sum_kernel, n_col),
        name="gather_sum",
        out_shape=jax.ShapeDtypeStruct((2, rows, dim), F32),
        in_specs=[pl.BlockSpec(memory_space=pltpu.VMEM)],
        out_specs=pl.BlockSpec(memory_space=pltpu.VMEM),
        scratch_shapes=[
            pltpu.VMEM((2, 2, n_col, rows, wide), F32),
            block(2, 2), block(2, 2), block(2), block(2), block(2), block(2), block(), block(),
            pltpu.VMEM((n_col, rows, wide), F32),
            pltpu.VMEM((n_col - 1, rows, wide), F32),
            dma((7 + n_col,)), dma((7 + n_col,)),
        ],
        compiler_params=pltpu.CompilerParams(collective_id=1, has_side_effects=True),
    )(acc.reshape(2, 2, 2, n_col, rows, wide))


def edge_kernel(
    group, src_i, dst_i, rel_i, neg_i, rel_row, rel_tab, src_all, dst_all,
    loss, acc, stage, s_tab, o_tab, w_tab, gs, go, gw, neg, qb, pos, term, stage_sem, neg_sem,
):
    n_src, n_dst = src_all.shape[0], dst_all.shape[0]
    ent = src_all.shape[2]
    n_rel = rel_tab.shape[1]
    groups = neg_i.shape[0]
    per = ent // NEGB
    sub = 128

    def neg_copy(g):
        b = neg_i[g]
        return pltpu.make_async_copy(
            dst_all.at[b // per, :, pl.ds(pl.multiple_of((b % per) * NEGB, NEGB), NEGB), :],
            neg.at[g % 2], neg_sem.at[g % 2],
        )

    def fill(table, base, read, rows):
        def step(i, carry):
            row = pl.multiple_of(i * sub, sub)
            for part in range(2):
                for half in range(2):
                    piece = read(part, row, half).astype(F32)
                    table[pl.ds(base + row * 4 + part * 2 + half, sub, stride=4), :] = piece
            return carry

        lax.fori_loop(0, rows // sub, step, 0)

    def load(all_ref, table, count):
        def copy(i):
            return pltpu.make_async_copy(all_ref.at[i], stage.at[i % 2], stage_sem.at[i % 2])

        copy(0).start()

        def step(i, carry):
            @pl.when(i + 1 < count)
            def _():
                copy(i + 1).start()

            copy(i).wait()
            slot = i % 2
            fill(
                table, i * (ent * 4),
                lambda part, row, half: stage[slot, part, pl.ds(row, sub), half * LANE : (half + 1) * LANE], ent,
            )
            return carry

        lax.fori_loop(0, count, step, 0)

    neg_copy(0).start()
    fill(w_tab, 0, lambda part, row, half: rel_tab[part, pl.ds(row, sub), half * LANE : (half + 1) * LANE], n_rel)
    load(src_all, s_tab, n_src)
    load(dst_all, o_tab, n_dst)

    eye = lax.broadcasted_iota(jnp.int32, (sub, LANE), 0) == lax.broadcasted_iota(jnp.int32, (sub, LANE), 1)
    nt = (((1,), (1,)), ((), ()))

    def one_group(g, carry):
        @pl.when(g + 1 < groups)
        def _():
            neg_copy(g + 1).start()

        def pick(i, inner):
            got = []
            for u in range(16):
                e = i * 16 + u
                a = pl.multiple_of(src_i[g * group + e] * 4, 4)
                b = pl.multiple_of(dst_i[g * group + e] * 4, 4)
                k = pl.multiple_of(rel_i[g * group + e] * 4, 4)
                got.append((s_tab[pl.ds(a, 4), :], o_tab[pl.ds(b, 4), :], w_tab[pl.ds(k, 4), :]))
            for u in range(16):
                at = pl.ds(pl.multiple_of((i * 16 + u) * 4, 4), 4)
                gs[at, :], go[at, :], gw[at, :] = got[u]
            return inner

        lax.fori_loop(0, group // 16, pick, 0)

        qrows = 32

        def query(i, inner):
            row = pl.multiple_of(i * qrows, qrows)
            score = None
            for half in range(2):
                part = lambda ref, p: ref[pl.ds(row * 4 + p * 2 + half, qrows, stride=4), :]
                sr, si, wr, wi = part(gs, 0), part(gs, 1), part(gw, 0), part(gw, 1)
                qr = sr * wr - si * wi
                qi = sr * wi + si * wr
                add = qr * part(go, 0) + qi * part(go, 1)
                score = add if score is None else score + add
                qb[pl.ds(row, qrows), half * LANE : (half + 1) * LANE] = qr.astype(BF16)
                qb[pl.ds(row, qrows), WIDE + half * LANE : WIDE + (half + 1) * LANE] = qi.astype(BF16)
            pos[pl.ds(row, qrows), :] = jnp.sum(score, 1, keepdims=True)
            return inner

        lax.fori_loop(0, group // qrows, query, 0)
        neg_copy(g).wait()
        slot = g % 2

        def block(i, inner):
            row = pl.multiple_of(i * sub, sub)
            rows = pl.ds(row, sub)
            n_re, n_im = neg[slot, 0], neg[slot, 1]
            score = lax.dot_general(qb[rows, :WIDE], n_re, nt, preferred_element_type=F32)
            score = score + lax.dot_general(qb[rows, WIDE:], n_im, nt, preferred_element_type=F32)
            small = jnp.exp(-jnp.abs(score))
            soft = jnp.maximum(score, 0.0) + jnp.log1p(small)
            weight = (jnp.where(score >= 0.0, 1.0, small) / (1.0 + small) * (1.0 / NEGB)).astype(BF16)
            p = pos[rows, :]
            p_small = jnp.exp(-jnp.abs(p))
            value = jnp.maximum(-p, 0.0) + jnp.log1p(p_small) + jnp.sum(soft, 1, keepdims=True) * (1.0 / NEGB)
            pull = jnp.where(p >= 0.0, p_small, 1.0) / (1.0 + p_small)
            loss[pl.ds(g * (group // sub) + i, 1), :] = jnp.sum(jnp.where(eye, value, 0.0), 0, keepdims=True)
            g_re = jnp.dot(weight, n_re, preferred_element_type=F32)
            g_im = jnp.dot(weight, n_im, preferred_element_type=F32)
            for half in range(2):
                part = lambda ref, q: ref[pl.ds(row * 4 + q * 2 + half, sub, stride=4), :]
                cols = slice(half * LANE, (half + 1) * LANE)
                d_re = g_re[:, cols] - pull * part(go, 0)
                d_im = g_im[:, cols] - pull * part(go, 1)
                s_re, s_im = part(gs, 0), part(gs, 1)
                at = pl.ds(pl.multiple_of(g * group + row, sub), sub)
                term[at, half * LANE : (half + 1) * LANE] = (d_re * s_re + d_im * s_im).astype(BF16)
                term[at, WIDE + half * LANE : WIDE + (half + 1) * LANE] = (d_im * s_re - d_re * s_im).astype(BF16)
            return inner

        lax.fori_loop(0, group // sub, block, 0)
        return carry

    lax.fori_loop(0, groups, one_group, 0)

    tile = 256
    edges = term.shape[0]

    def reduce(i, carry):
        row = pl.multiple_of(i * tile, tile)
        ids = lax.broadcasted_iota(jnp.int32, (tile, edges), 0) + row
        hot = jnp.where(ids == rel_row[...], 1.0, 0.0).astype(BF16)
        acc[pl.ds(row, tile), :] = jnp.dot(hot, term[...], preferred_element_type=F32)
        return carry

    lax.fori_loop(0, n_rel // tile, reduce, 0)


def edge_terms(src_all, dst_all, relations, src_index, dst_index, rel_index, neg_block):
    edges, groups = src_index.shape[0], neg_block.shape[0]
    group = edges // groups
    n_rel = relations.shape[1]
    ent = src_all.shape[2]
    smem = pl.BlockSpec(memory_space=pltpu.SMEM)
    vmem = pl.BlockSpec(memory_space=pltpu.VMEM)
    hbm = pl.BlockSpec(memory_space=pltpu.HBM)
    quad = 4
    return pl.pallas_call(
        functools.partial(edge_kernel, group),
        name="edge_terms",
        out_shape=(
            jax.ShapeDtypeStruct((edges // LANE, LANE), F32),
            jax.ShapeDtypeStruct((n_rel, 2 * WIDE), F32),
        ),
        in_specs=[smem, smem, smem, smem, vmem, vmem, hbm, hbm],
        out_specs=(vmem, vmem),
        scratch_shapes=[
            pltpu.VMEM((2, 2, ent, WIDE), BF16),
            pltpu.VMEM((src_all.shape[0] * ent * quad, LANE), F32),
            pltpu.VMEM((dst_all.shape[0] * ent * quad, LANE), F32),
            pltpu.VMEM((n_rel * quad, LANE), F32),
            pltpu.VMEM((group * quad, LANE), F32),
            pltpu.VMEM((group * quad, LANE), F32),
            pltpu.VMEM((group * quad, LANE), F32),
            pltpu.VMEM((2, 2, NEGB, WIDE), BF16),
            pltpu.VMEM((group, 2 * WIDE), BF16),
            pltpu.VMEM((group, 1), F32),
            pltpu.VMEM((edges, 2 * WIDE), BF16),
            pltpu.SemaphoreType.DMA((2,)),
            pltpu.SemaphoreType.DMA((2,)),
        ],
        compiler_params=pltpu.CompilerParams(vmem_limit_bytes=62 * 2**20),
    )(
        src_index, dst_index, rel_index, neg_block, rel_index.reshape(1, edges), relations, src_all, dst_all,
    )


def body(n_row, n_col, entities, relations, src_index, dst_index, rel_index, neg_block):
    dim = entities.shape[2]
    ent = entities.shape[1]
    pad = ((0, 0), (0, 0), (0, WIDE - dim))
    if n_row != 8 or n_col != 4 or (n_row + n_col) * ent * 4 * LANE * 4 > 36 * 2**20:
        return wide_body(entities, relations, src_index, dst_index, rel_index, neg_block)
    src_all, dst_all = spread(n_row, n_col, jnp.pad(entities, pad))
    edge_loss, acc = edge_terms(
        src_all, dst_all, jnp.pad(relations, pad), src_index, dst_index, rel_index, neg_block
    )
    grad = gather_sum(n_row, n_col, acc, dim)
    return edge_loss.reshape(-1), grad


def bucket_terms(picked_src, picked_dst, negatives, relations, rel_ids):
    onehot = (rel_ids[:, None] == jnp.arange(relations.shape[1], dtype=jnp.int32)[None, :]).astype(
        jnp.bfloat16
    )
    rel_re = jnp.dot(onehot, relations[0], preferred_element_type=jnp.float32)
    rel_im = jnp.dot(onehot, relations[1], preferred_element_type=jnp.float32)
    src_re = picked_src[0].astype(jnp.float32)
    src_im = picked_src[1].astype(jnp.float32)
    dst_re = picked_dst[0].astype(jnp.float32)
    dst_im = picked_dst[1].astype(jnp.float32)
    query_re = src_re * rel_re - src_im * rel_im
    query_im = src_re * rel_im + src_im * rel_re
    pos_score = jnp.sum(query_re * dst_re, 1) + jnp.sum(query_im * dst_im, 1)
    groups = negatives.shape[1]
    dim = query_re.shape[1]
    qre_b = query_re.astype(jnp.bfloat16).reshape(groups, -1, dim)
    qim_b = query_im.astype(jnp.bfloat16).reshape(groups, -1, dim)
    neg_score = jnp.einsum(
        "kcd,knd->kcn", qre_b, negatives[0], preferred_element_type=jnp.float32
    ) + jnp.einsum("kcd,knd->kcn", qim_b, negatives[1], preferred_element_type=jnp.float32)
    edge_loss = jax.nn.softplus(-pos_score) + jnp.mean(jax.nn.softplus(neg_score), -1).reshape(-1)
    weights = (jax.nn.sigmoid(neg_score) / NEGB).astype(jnp.bfloat16)
    gneg_re = jnp.einsum(
        "kcn,knd->kcd", weights, negatives[0], preferred_element_type=jnp.float32
    ).reshape(-1, dim)
    gneg_im = jnp.einsum(
        "kcn,knd->kcd", weights, negatives[1], preferred_element_type=jnp.float32
    ).reshape(-1, dim)
    pull = jax.nn.sigmoid(-pos_score)[:, None]
    grad_re = gneg_re - pull * dst_re
    grad_im = gneg_im - pull * dst_im
    term_re = (grad_re * src_re + grad_im * src_im).astype(jnp.bfloat16)
    term_im = (grad_im * src_re - grad_re * src_im).astype(jnp.bfloat16)
    dims = (((0,), (0,)), ((), ()))
    rel_grad = jnp.stack(
        [
            lax.dot_general(onehot, term_re, dims, preferred_element_type=jnp.float32),
            lax.dot_general(onehot, term_im, dims, preferred_element_type=jnp.float32),
        ],
        0,
    )
    return (edge_loss, rel_grad)


def wide_body(entities, relations, src_index, dst_index, rel_index, neg_block):
    dim = entities.shape[2]
    source_rows = lax.all_gather(entities, "col", axis=1, tiled=True)
    picked_src = jnp.take(source_rows, src_index, axis=1)
    target_rows = lax.all_gather(entities, "row", axis=1, tiled=True)
    picked_dst = jnp.take(target_rows, dst_index, axis=1)
    negatives = jnp.take(target_rows.reshape(2, -1, NEGB, dim), neg_block, axis=1)
    edge_loss, rel_grad = bucket_terms(picked_src, picked_dst, negatives, relations, rel_index)
    row_share = lax.psum_scatter(rel_grad, "row", scatter_dimension=1, tiled=True)
    grad_share = lax.psum_scatter(row_share, "col", scatter_dimension=1, tiled=True)
    return (edge_loss, grad_share)


def solution(mesh):
    placed = (
        P(None, ("row", "col"), None),
        P(),
        P(("row", "col")),
        P(("row", "col")),
        P(("row", "col")),
        P(("row", "col")),
    )
    return jax.shard_map(
        functools.partial(body, mesh.shape["row"], mesh.shape["col"]),
        mesh=mesh,
        in_specs=placed,
        out_specs=(P(("row", "col")), P(None, ("row", "col"), None)),
        check_vma=False,
    )
```
